512 devices in a mesh: section: 4 (over x), wide: 32 (over y_hi, z, core), narrow: 4 (over y_lo).
Axes of the slice: x: 4, y: 8 (y_hi: 2, y_lo: 4; y = y_hi * 4 + y_lo), z: 8, core: 2. Of those that a mesh axis runs over, the one named last changes fastest.
Arguments:
- valence_orbitals: float32 [8, 48, 2304], P(None, 'narrow'), may hold values from -6 to 6
- conduction_orbitals: float32 [128, 48, 2304], P(('section', 'wide'), 'narrow'), may hold values from -6 to 6
- valence_energy: float32 [8], replicated, may hold values from -7 to -1
- conduction_energy: float32 [128], replicated, may hold values from 1 to 7
- frequency: float32 [1], replicated, may hold values from 0.5 to 4
- pair_bands: int32 [512, 2], P(('section', 'wide')), may hold values from 0 to 127, as said below
- gvec_index: int32 [12288], replicated, may hold values from 0 to 110591, as said below
Outputs:
- chi: float32 [12288, 12288], P(('section', 'narrow'), 'wide')
The draws below stay inside these ranges and needn't reach their ends.
Inputs may be any that keep to these rules, and one draw needn't show every extreme that they name: `pair_bands`: column 0 is a valence band, column 1 a conduction band; rows b * 4 to (b + 1) * 4 - 1 pair conduction band b with 4 distinct valence bands. `gvec_index`: the 12288 indices are distinct.
All inputs are finite; a program needn't handle non-finite values.
Results may differ from the reference program's by a relative error of at most 0.000094.
Values sent between devices are 32-bit elements; how exact they have to be, the bound alone decides.
A program may use at most 192 MiB of HBM per device.

```python
import math
import jax
import jax.numpy as jnp
from jax import lax

GRID = 48
NG = 12288
NV = 8
PV = 4
NC = 128
PAIRS = 512
N_SECTION = 4
N_WIDE = 32


def draw_gvec_index(key, part):
    order = jax.random.permutation(jax.random.fold_in(key, 17), GRID * GRID * GRID)
    return order[:NG].astype(jnp.int32)


def draw_pair_bands(key, part):
    band_keys = jax.random.split(jax.random.fold_in(key, 29), NC)
    valence_part = jax.vmap(lambda one_key: jax.random.permutation(one_key, NV)[:PV])(band_keys).astype(jnp.int32)
    conduction_part = jnp.broadcast_to(jnp.arange(NC, dtype=jnp.int32)[:, None], (NC, PV))
    return jnp.stack([valence_part, conduction_part], axis=2).reshape(NC * PV, 2)


def block_scale(key, extent, cuts, smallest, high):
    level, own = 1.0, jax.random.fold_in(key, 6)
    for dim, shards_of in cuts:
        steps = jnp.exp(jax.random.uniform(jax.random.fold_in(own, dim), (shards_of,), jnp.float32, smallest / len(cuts), high / len(cuts)))
        level = level * jnp.repeat(steps, extent[dim] // shards_of).reshape([-1 if axis == dim else 1 for axis in range(len(extent))])
    return level


def gaussian(rng, extent, scale, reach, pieces=(), held_as=jnp.bfloat16):
    drawn = jax.random.normal(rng, extent, jnp.float32) * scale
    if len(pieces) > 0:
        drawn = block_scale(rng, extent, pieces, -0.22, 0.18) * drawn
    return jnp.clip(drawn, min=-reach, max=reach).astype(held_as)


def setup_inputs(seed: int = 0) -> dict:
    arg_keys = jax.random.split(jax.random.key(seed), 8)
    return {
        "valence_orbitals": gaussian(arg_keys[0], (NV, GRID, GRID * GRID), 1.0, 6.0, ((1, 4),), jnp.float32),
        "conduction_orbitals": gaussian(arg_keys[1], (NC, GRID, GRID * GRID), 1.0, 6.0, ((0, 128), (1, 4)), jnp.float32),
        "valence_energy": jnp.clip(jax.random.uniform(arg_keys[2], (NV,), jnp.float32, -7.0, -1.0), -7.0, -1.0),
        "conduction_energy": jnp.clip(jax.random.uniform(arg_keys[3], (NC,), jnp.float32, 1.0, 7.0), 1.0, 7.0),
        "frequency": jnp.clip(jax.random.uniform(arg_keys[4], (1,), jnp.float32, 0.5, 4.0), 0.5, 4.0),
        "pair_bands": draw_pair_bands(jax.random.fold_in(arg_keys[7], 71), 0),
        "gvec_index": draw_gvec_index(jax.random.fold_in(arg_keys[7], 71), 0),
    }


def build_cosine(length):
    wavenumber = jnp.arange(length, dtype=jnp.float32)[:, None]
    position = jnp.arange(length, dtype=jnp.float32)[None, :]
    cosine = math.sqrt(2.0 / length) * jnp.cos(math.pi * (2.0 * position + 1.0) * wavenumber / (2.0 * length))
    return jnp.where(wavenumber == 0.0, cosine * math.sqrt(0.5), cosine)

def reference(valence_orbitals, conduction_orbitals, valence_energy, conduction_energy, frequency, pair_bands, gvec_index):
    cosine = build_cosine(GRID)
    highest = lax.Precision.HIGHEST

    def one_block(band_pairs):
        valence_pick = valence_orbitals[band_pairs[:, 0]].reshape(-1, GRID, GRID, GRID)
        conduction_pick = conduction_orbitals[band_pairs[:, 1]].reshape(-1, GRID, GRID, GRID)
        density = valence_pick * conduction_pick
        sweep_one = jnp.einsum('pxyz,kz->pxyk', density, cosine, precision=highest)
        sweep_two = jnp.einsum('pxyk,jy->pxjk', sweep_one, cosine, precision=highest)
        sweep_three = jnp.einsum('pxjk,ix->pijk', sweep_two, cosine, precision=highest)
        return sweep_three.reshape(sweep_three.shape[0], -1)[:, gvec_index]
    blocks = pair_bands.reshape(N_SECTION * N_WIDE, PV, 2)
    coefficients = lax.map(one_block, blocks).reshape(PAIRS, NG)
    energy_gap = conduction_energy[pair_bands[:, 1]] - valence_energy[pair_bands[:, 0]]
    weight = -4.0 * energy_gap / (energy_gap * energy_gap + frequency[0] * frequency[0]) / math.sqrt(PAIRS)
    weighted = coefficients * weight[:, None]
    return lax.dot_general(weighted, coefficients, (((0,), (0,)), ((), ())), precision=highest, preferred_element_type=jnp.float32)
```

```python
import functools
import math

import jax
import jax.numpy as jnp
import numpy as np
from jax import lax
from jax.experimental import pallas as pl
from jax.experimental.pallas import tpu as pltpu
from jax.sharding import PartitionSpec as P

F32, BF16 = jnp.float32, jnp.bfloat16
MESH = pl.DeviceIdType.MESH
GRID, NARROW, SECTION = 48, 4, 4
HIGH, RING, CORES = 2, 8, 2
WIDE = HIGH * RING * CORES
PLANES = GRID // NARROW
AREA = GRID * GRID
VECTORS = 12288
ROWS, COLS = VECTORS // 16, VECTORS // 32


def split_np(a):
    a = np.asarray(a, np.float32)
    h = a.astype(BF16)
    return h, (a - h.astype(np.float32)).astype(BF16)


def tables():
    k, x = np.arange(GRID)[:, None], np.arange(GRID)[None, :]
    c = math.sqrt(2.0 / GRID) * np.cos(math.pi * (2 * x + 1) * k / (2 * GRID))
    c[0] *= math.sqrt(0.5)
    cx = np.zeros((64, GRID))
    order = [p * PLANES + q for p in range(4) for q in range(8)] + [p * PLANES + q for p in range(4) for q in range(8, 12)]
    for i in range(GRID):
        cx[(i // 6) * 8 + i % 6] = c[i, order]
    h, l = split_np(cx)
    cx3 = np.concatenate([h, l, h], axis=1)
    bh, bl = split_np(np.kron(np.eye(16), c.T))
    h, l = split_np(c)
    cy3 = np.concatenate([h, l, h], axis=1)
    return cx3, bh, bl, cy3


def hi_lo(a):
    h = a.astype(BF16)
    return h, (a - h.astype(F32)).astype(BF16)


def dot(a, b):
    return lax.dot_general(a, b, (((1,), (0,)), ((), ())), preferred_element_type=F32)


def exchange_body(
    bands_ref, valence_ref, conduction_ref, out8_ref, out4_ref, stage8_ref, stage4_ref, send_sem, recv_sem
):
    me = lax.axis_index("narrow")
    barrier = pltpu.get_barrier_semaphore()
    for d in range(1, NARROW):
        pl.semaphore_signal(
            barrier, inc=1, device_id={"narrow": lax.rem(me + d, NARROW)}, device_id_type=MESH
        )
    conduction = conduction_ref[0]
    for p in range(NARROW):
        density = valence_ref[bands_ref[p, 0]] * conduction
        stage8_ref[p] = density[:8]
        stage4_ref[p] = density[8:]
    out8_ref[me] = stage8_ref[me]
    out4_ref[me] = stage4_ref[me]
    pl.semaphore_wait(barrier, NARROW - 1)
    copies = []
    for d in range(1, NARROW):
        peer = lax.rem(me + d, NARROW)
        for part, (src, dst) in enumerate(((stage8_ref, out8_ref), (stage4_ref, out4_ref))):
            copy = pltpu.make_async_remote_copy(
                src_ref=src.at[peer],
                dst_ref=dst.at[me],
                send_sem=send_sem.at[part, d - 1],
                recv_sem=recv_sem.at[part, d - 1],
                device_id={"narrow": peer},
                device_id_type=MESH,
            )
            copy.start()
            copies.append(copy)
    for copy in copies:
        copy.wait()


def exchange(bands, valence, conduction):
    return pl.pallas_call(
        exchange_body,
        out_shape=(
            jax.ShapeDtypeStruct((NARROW, 8, AREA), F32),
            jax.ShapeDtypeStruct((NARROW, 4, AREA), F32),
        ),
        in_specs=[
            pl.BlockSpec(memory_space=pltpu.SMEM),
            pl.BlockSpec(memory_space=pltpu.VMEM),
            pl.BlockSpec(memory_space=pltpu.VMEM),
        ],
        out_specs=(pl.BlockSpec(memory_space=pltpu.VMEM), pl.BlockSpec(memory_space=pltpu.VMEM)),
        scratch_shapes=[
            pltpu.VMEM((NARROW, 8, AREA), F32),
            pltpu.VMEM((NARROW, 4, AREA), F32),
            pltpu.SemaphoreType.DMA((2, NARROW - 1)),
            pltpu.SemaphoreType.DMA((2, NARROW - 1)),
        ],
        compiler_params=pltpu.CompilerParams(collective_id=0, has_side_effects=True),
        name="exchange",
    )(bands, valence, conduction)


def coefficients_body(
    bands_ref, ve_ref, ce_ref, freq_ref, d8_ref, d4_ref, rid_ref, lid_ref, cx_ref, bh_ref, bl_ref, cy_ref,
    row_ref, col_ref, z_ref, s_ref, t_ref, tt_ref,
):
    me = lax.axis_index("narrow")
    valence = jnp.full((1, ROWS), ve_ref[bands_ref[me, 0]], F32)
    conduction = jnp.full((1, ROWS), ce_ref[bands_ref[me, 1]], F32)
    frequency = jnp.full((1, ROWS), freq_ref[0], F32)
    gap = conduction - valence
    weight = -4.0 * gap / (gap * gap + frequency * frequency) / math.sqrt(512.0)

    last = [jnp.concatenate([d4_ref[2 * q], d4_ref[2 * q + 1]], axis=0) for q in range(2)]
    dh, dl = hi_lo(jnp.concatenate([d8_ref[...].reshape(32, AREA), *last], axis=0))
    a = dot(cx_ref[...], jnp.concatenate([dh, dh, dl], axis=0))
    ah, al = hi_lo(a)
    third = AREA // 3
    lhs = jnp.concatenate(
        [half[:, b * third : (b + 1) * third] for half in (ah, al) for b in range(3)], axis=0
    )
    by_high = dot(lhs, bh_ref[...])
    by_low = dot(lhs[:192], bl_ref[...])
    for b in range(3):
        rows = slice(b * 64, (b + 1) * 64)
        z_ref[:, b * third : (b + 1) * third] = (
            by_high[rows] + by_high[192 + b * 64 : 256 + b * 64] + by_low[rows]
        )

    def relay(group, carry):
        part = z_ref[:, pl.ds(pl.multiple_of(group * 384, 128), 384)]
        for y in range(8):
            s_ref[group * 8 + y] = jnp.concatenate(
                [part[i * 8 : (i + 1) * 8, y * GRID : (y + 1) * GRID] for i in range(8)], axis=1
            )
        return carry

    lax.fori_loop(0, 6, relay, 0)
    for r in range(6):
        sh, sl = hi_lo(s_ref[:, r, :])
        t = dot(cy_ref[...], jnp.concatenate([sh, sh, sl], axis=0))
        for u in range(3):
            t_ref[(r * 3 + u) * GRID : (r * 3 + u + 1) * GRID, :] = t[:, u * 128 : (u + 1) * 128]
    th, tl = hi_lo(t_ref[...].T)
    tt_ref[0:128, :864] = th
    tt_ref[128:256, :864] = tl

    def chunk(k, carry):
        parts = []
        for q in range(3):
            here = pl.ds(pl.multiple_of(k * ROWS + q * 256, 256), 256)
            rid, lid = rid_ref[0:1, here], lid_ref[0:1, here]
            acc = None
            for kt in range(4):
                kn = min(256, 864 - kt * 256)
                index = lax.broadcasted_iota(jnp.int32, (kn, 256), 0) + kt * 256
                hot = jnp.where(index == rid, 1.0, 0.0).astype(BF16)
                part = dot(tt_ref[:, kt * 256 : kt * 256 + kn], hot)
                acc = part if acc is None else acc + part
            both = acc[:128] + acc[128:]
            mine = lax.broadcasted_iota(jnp.int32, (128, 256), 0) == lid
            parts.append(jnp.sum(jnp.where(mine, both, 0.0), axis=0, keepdims=True))
        c = jnp.concatenate(parts, axis=1)
        row_ref[k] = c * weight
        col_ref[2 * k] = c[:, :COLS]
        col_ref[2 * k + 1] = c[:, COLS:]
        return carry

    lax.fori_loop(0, 16, chunk, 0)


def coefficients(bands, ve, ce, freq, d8, d4, rid, lid):
    smem, vmem = pl.BlockSpec(memory_space=pltpu.SMEM), pl.BlockSpec(memory_space=pltpu.VMEM)
    return pl.pallas_call(
        coefficients_body,
        out_shape=(
            jax.ShapeDtypeStruct((16, 1, ROWS), F32),
            jax.ShapeDtypeStruct((32, 1, COLS), F32),
        ),
        in_specs=[smem] * 4 + [vmem] * 8,
        out_specs=(vmem, vmem),
        scratch_shapes=[
            pltpu.VMEM((64, AREA), F32),
            pltpu.VMEM((GRID, 8, 384), F32),
            pltpu.VMEM((864, 128), F32),
            pltpu.VMEM((256, 896), BF16),
        ],
        compiler_params=pltpu.CompilerParams(vmem_limit_bytes=40 * 1024 * 1024),
        name="coefficients",
    )(bands, ve, ce, freq, d8, d4, rid, lid, *[jnp.asarray(t) for t in tables()])


def gather_body(row_ref, col_ref, rows_ref, cols_ref, cbuf_ref, send_small, send_row, send_side, send_col,
                recv_row1, recv_col1, recv_ring, recv_side, recv_y, recv_x, recv_xx):
    s, w, n = lax.axis_index("section"), lax.axis_index("wide"), lax.axis_index("narrow")
    yh, z, c = w // 16, lax.rem(w // 2, RING), lax.rem(w, 2)
    barrier = pltpu.get_barrier_semaphore()

    def row_peer(d):
        sp, np_ = lax.rem(s + lax.rem(d, 4), 4), lax.rem(n + lax.rem(d // 4, 4), 4)
        wp = lax.rem(yh + d // 16, 2) * 16 + z * 2 + c
        return sp, wp, np_

    def col_peer(d):
        return lax.rem(w + d, WIDE)

    def greet(d, carry):
        sp, wp, np_ = row_peer(d)
        pl.semaphore_signal(barrier, inc=1, device_id={"section": sp, "wide": wp, "narrow": np_}, device_id_type=MESH)
        pl.semaphore_signal(barrier, inc=1, device_id={"wide": col_peer(d)}, device_id_type=MESH)
        return carry

    lax.fori_loop(1, 32, greet, 0)
    block = (z * 2 + c) * 32
    home = block + yh * 16 + s * 4 + n
    from_me = (z * 2 + c) * 2 + yh
    rows_ref[home] = row_ref[s * 4 + n]
    cbuf_ref[from_me] = col_ref[w]
    pl.semaphore_wait(barrier, 62)

    def spread(d, carry):
        sp, wp, np_ = row_peer(d)
        pltpu.make_async_remote_copy(
            src_ref=row_ref.at[sp * 4 + np_], dst_ref=rows_ref.at[home], send_sem=send_small,
            recv_sem=recv_row1.at[d // 16],
            device_id={"section": sp, "wide": wp, "narrow": np_}, device_id_type=MESH,
        ).start()
        wc = col_peer(d)
        pltpu.make_async_remote_copy(
            src_ref=col_ref.at[wc], dst_ref=cbuf_ref.at[from_me], send_sem=send_small,
            recv_sem=recv_col1, device_id={"wide": wc}, device_id_type=MESH,
        ).start()
        return carry

    lax.fori_loop(1, 32, spread, 0)

    def sub(zz, cc, h):
        return rows_ref.at[pl.ds((zz * 2 + cc) * 32 + lax.rem(yh + h, 2) * 16, 16)]

    def ring_peer(step):
        return yh * 16 + lax.rem(z + step + RING, RING) * 2 + c

    side = yh * 16 + z * 2 + (1 - c)
    sends = []

    def send(ref, send_sem, recv_sem, **device):
        copy = pltpu.make_async_remote_copy(
            src_ref=ref, dst_ref=ref, send_sem=send_sem, recv_sem=recv_sem, device_id=device, device_id_type=MESH
        )
        copy.start()
        sends.append(copy)

    def arrived(ref, sem):
        pltpu.make_async_copy(ref, ref, sem).wait()

    arrived(cbuf_ref.at[pl.ds(0, 31)], recv_col1)
    own_cols = cols_ref.at[s * 4 + n]
    cols_ref[s * 4 + n] = cbuf_ref[...]
    for d in range(1, NARROW):
        copy = pltpu.make_async_remote_copy(
            src_ref=cbuf_ref, dst_ref=own_cols, send_sem=send_col, recv_sem=recv_y.at[d - 1],
            device_id={"narrow": lax.rem(n + d, NARROW)}, device_id_type=MESH,
        )
        copy.start()
        sends.append(copy)
    for i, step in enumerate((1, -1)):
        copy = pltpu.make_async_remote_copy(
            src_ref=cbuf_ref, dst_ref=own_cols, send_sem=send_col, recv_sem=recv_x.at[0, i],
            device_id={"section": lax.rem(s + step + SECTION, SECTION)}, device_id_type=MESH,
        )
        copy.start()
        sends.append(copy)

    for h in range(2):
        arrived(rows_ref.at[pl.ds(0, 15 + h)], recv_row1.at[h])
        send(sub(z, c, h), send_row, recv_ring.at[0, 0, h], wide=ring_peer(1))
        send(sub(z, c, h), send_row, recv_ring.at[1, 0, h], wide=ring_peer(-1))
        send(sub(z, c, h), send_side, recv_side.at[0, 0, h], wide=side)

    def cols_of(ds, d):
        return cols_ref.at[lax.rem(s + ds + SECTION, SECTION) * 4 + lax.rem(n - d + NARROW, NARROW)]

    for k in range(1, 5):
        if k < NARROW:
            got = cols_of(0, k)
            arrived(got, recv_y.at[k - 1])
            send(got, send_col, recv_x.at[k, 0], section=lax.rem(s + 1, SECTION))
            send(got, send_col, recv_x.at[k, 1], section=lax.rem(s + SECTION - 1, SECTION))
        for h in range(2):
            for i, step in ((0, 1), (1, -1)):
                if k == 4 and h != i:
                    continue
                got = sub(lax.rem(z - step * k + RING, RING), c, h)
                arrived(got, recv_ring.at[i, k - 1, h])
                if k < 3 or (k == 3 and h == i):
                    send(got, send_row, recv_ring.at[i, k, h], wide=ring_peer(step))
                send(got, send_side, recv_side.at[i, k, h], wide=side)
    for d in range(NARROW):
        i, step = (0, 1) if d % 2 == 0 else (1, -1)
        got = cols_of(-step, d)
        arrived(got, recv_x.at[d, i])
        send(got, send_col, recv_xx.at[d], section=lax.rem(s + step + SECTION, SECTION))
    for d in range(NARROW):
        i, step = (1, -1) if d % 2 == 0 else (0, 1)
        arrived(cols_of(-step, d), recv_x.at[d, i])
        arrived(cols_of(2, d), recv_xx.at[d])
    for h in range(2):
        arrived(sub(z, 1 - c, h), recv_side.at[0, 0, h])
        for k in range(1, 5):
            for i, step in ((0, 1), (1, -1)):
                if k == 4 and h != i:
                    continue
                arrived(sub(lax.rem(z - step * k + RING, RING), 1 - c, h), recv_side.at[i, k, h])
    for copy in sends:
        copy.wait_send()
    arrived(rows_ref.at[pl.ds(0, 31)], send_small)
    arrived(cbuf_ref.at[pl.ds(0, 31)], send_small)


def gather(row, col):
    vmem = pl.BlockSpec(memory_space=pltpu.VMEM)
    dma = pltpu.SemaphoreType.DMA
    return pl.pallas_call(
        gather_body,
        out_shape=(
            jax.ShapeDtypeStruct((512, 1, ROWS), F32),
            jax.ShapeDtypeStruct((16, WIDE, 1, COLS), F32),
        ),
        in_specs=[vmem, vmem],
        out_specs=(vmem, vmem),
        scratch_shapes=[
            pltpu.VMEM((WIDE, 1, COLS), F32),
            dma, dma, dma, dma,
            dma((2,)), dma, dma((2, 4, 2)), dma((2, 5, 2)), dma((3,)), dma((4, 2)), dma((4,)),
        ],
        compiler_params=pltpu.CompilerParams(collective_id=1, has_side_effects=True),
        name="gather",
    )(row, col)


def product_body(rows_ref, cols_ref, out_ref):
    right = jnp.concatenate([cols_ref[pl.ds(u, 512, stride=3), :] for u in range(3)], axis=1)
    bh, bl = hi_lo(right)
    for t in range(6):
        left = jnp.concatenate(
            [rows_ref[pl.ds(sn * 6 + t, 32, stride=96), :] for sn in range(16)], axis=0
        )
        ah, al = hi_lo(left.T)
        out_ref[t * 128 : (t + 1) * 128, :] = dot(
            jnp.concatenate([ah, ah, al], axis=1), jnp.concatenate([bh, bl, bh], axis=0)
        )


def product(rows, cols):
    return pl.pallas_call(
        product_body,
        out_shape=jax.ShapeDtypeStruct((ROWS, COLS), F32),
        compiler_params=pltpu.CompilerParams(vmem_limit_bytes=40 * 1024 * 1024),
        name="product",
    )(rows.reshape(512 * 6, 128), cols.reshape(512 * 3, 128))


def on_device(ve_orb, ce_orb, ve, ce, freq, bands, gvec):
    i, j, k = gvec // AREA, lax.rem(gvec // GRID, GRID), lax.rem(gvec, GRID)
    lane = (i // 6) * GRID + k
    rid = ((lax.rem(i, 6) * 3 + lane // 128) * GRID + j).reshape(1, -1)
    lid = lax.rem(lane, 128).reshape(1, -1)
    d8, d4 = exchange(bands, ve_orb, ce_orb)
    row, col = coefficients(bands, ve, ce, freq, d8, d4, rid, lid)
    rows, cols = gather(row, col)
    return product(rows, cols)


def solution(mesh):
    in_specs = (
        P(None, "narrow", None),
        P(("section", "wide"), "narrow", None),
        P(),
        P(),
        P(),
        P(("section", "wide"), None),
        P(),
    )
    return jax.shard_map(
        on_device,
        mesh=mesh,
        in_specs=in_specs,
        out_specs=P(("section", "narrow"), "wide"),
        check_vma=False,
    )
```

```python
import functools
import math

import jax
import jax.numpy as jnp
import numpy as np
from jax import lax
from jax.experimental import pallas as pl
from jax.experimental.pallas import tpu as pltpu
from jax.sharding import PartitionSpec as P

F32, BF16 = jnp.float32, jnp.bfloat16
MESH = pl.DeviceIdType.MESH
GRID, NARROW, SECTION = 48, 4, 4
HIGH, RING, CORES = 2, 8, 2
WIDE = HIGH * RING * CORES
PLANES = GRID // NARROW
AREA = GRID * GRID
VECTORS = 12288
ROWS, COLS = VECTORS // 16, VECTORS // 32


def split_np(a):
    a = np.asarray(a, np.float32)
    h = a.astype(BF16)
    return h, (a - h.astype(np.float32)).astype(BF16)


def tables():
    k, x = np.arange(GRID)[:, None], np.arange(GRID)[None, :]
    c = math.sqrt(2.0 / GRID) * np.cos(math.pi * (2 * x + 1) * k / (2 * GRID))
    c[0] *= math.sqrt(0.5)
    cx = np.zeros((64, GRID))
    order = [p * PLANES + q for p in range(4) for q in range(8)] + [p * PLANES + q for p in range(4) for q in range(8, 12)]
    for i in range(GRID):
        cx[(i // 6) * 8 + i % 6] = c[i, order]
    h, l = split_np(cx)
    cx3 = np.concatenate([h, l, h], axis=1)
    bh, bl = split_np(np.kron(np.eye(16), c.T))
    h, l = split_np(c)
    cy3 = np.concatenate([h, l, h], axis=1)
    return cx3, bh, bl, cy3


def hi_lo(a):
    h = a.astype(BF16)
    return h, (a - h.astype(F32)).astype(BF16)


def dot(a, b):
    return lax.dot_general(a, b, (((1,), (0,)), ((), ())), preferred_element_type=F32)


def exchange_body(
    bands_ref, valence_ref, conduction_ref, out8_ref, out4_ref, stage8_ref, stage4_ref, send_sem, recv_sem
):
    me = lax.axis_index("narrow")
    barrier = pltpu.get_barrier_semaphore()
    for d in range(1, NARROW):
        pl.semaphore_signal(
            barrier, inc=1, device_id={"narrow": lax.rem(me + d, NARROW)}, device_id_type=MESH
        )
    for t in range(AREA // 128):
        conduction = conduction_ref[pl.ds(t, PLANES, stride=AREA // 128), :]
        lanes = slice(t * 128, (t + 1) * 128)
        for p in range(NARROW):
            valence = valence_ref[pl.ds(t * 8 + bands_ref[0, p], PLANES, stride=AREA // 16), :]
            density = valence * conduction
            stage8_ref[p, :, lanes] = density[:8]
            stage4_ref[p, :, lanes] = density[8:]
    out8_ref[me] = stage8_ref[me]
    out4_ref[me] = stage4_ref[me]
    pl.semaphore_wait(barrier, NARROW - 1)
    copies = []
    for d in range(1, NARROW):
        peer = lax.rem(me + d, NARROW)
        for part, (src, dst) in enumerate(((stage8_ref, out8_ref), (stage4_ref, out4_ref))):
            copy = pltpu.make_async_remote_copy(
                src_ref=src.at[peer],
                dst_ref=dst.at[me],
                send_sem=send_sem.at[part, d - 1],
                recv_sem=recv_sem.at[part, d - 1],
                device_id={"narrow": peer},
                device_id_type=MESH,
            )
            copy.start()
            copies.append(copy)
    for copy in copies:
        copy.wait()


def exchange(bands, valence, conduction):
    vmem = pl.BlockSpec(memory_space=pltpu.VMEM)
    return pl.pallas_call(
        exchange_body,
        out_shape=(
            jax.ShapeDtypeStruct((NARROW, 8, AREA), F32),
            jax.ShapeDtypeStruct((NARROW, 4, AREA), F32),
        ),
        in_specs=[pl.BlockSpec(memory_space=pltpu.SMEM), vmem, vmem],
        out_specs=(vmem, vmem),
        scratch_shapes=[
            pltpu.VMEM((NARROW, 8, AREA), F32),
            pltpu.VMEM((NARROW, 4, AREA), F32),
            pltpu.SemaphoreType.DMA((2, NARROW - 1)),
            pltpu.SemaphoreType.DMA((2, NARROW - 1)),
        ],
        compiler_params=pltpu.CompilerParams(
            collective_id=0, has_side_effects=True, vmem_limit_bytes=16 * 1024 * 1024
        ),
        cost_estimate=pl.CostEstimate(flops=10**10, bytes_accessed=2 * 10**7, transcendentals=0),
        name="exchange",
    )(bands, valence, conduction)


def polarize_body(
    bands_ref, ve_ref, ce_ref, freq_ref, d8_ref, d4_ref, gvec_ref, cx_ref, bh_ref, bl_ref, cy_ref,
    out_ref,
    rid_ref, lid_ref, z_ref, s_ref, t_ref, tt_ref, row_ref, col_ref, rows_ref, cols_ref, at_ref, bb_ref,
    send_small, send_row, send_side, send_col,
    recv_row1, recv_col1, recv_ring, recv_side, recv_y, recv_x, recv_xx,
):
    s, w, n = lax.axis_index("section"), lax.axis_index("wide"), lax.axis_index("narrow")
    yh, z, c = w // (RING * CORES), lax.rem(w // CORES, RING), lax.rem(w, CORES)
    me = s * NARROW + n

    def row_peer(d):
        sp, np_ = lax.rem(s + lax.rem(d, 4), SECTION), lax.rem(n + lax.rem(d // 4, 4), NARROW)
        wp = lax.rem(yh + d // 16, HIGH) * (RING * CORES) + z * CORES + c
        return sp, wp, np_

    def col_peer(d):
        return lax.rem(w + d, WIDE)

    barrier = pltpu.get_barrier_semaphore()

    def greet(d, carry):
        sp, wp, np_ = row_peer(d)
        pl.semaphore_signal(
            barrier, inc=1, device_id={"section": sp, "wide": wp, "narrow": np_}, device_id_type=MESH
        )
        pl.semaphore_signal(barrier, inc=1, device_id={"wide": col_peer(d)}, device_id_type=MESH)
        return carry

    lax.fori_loop(1, 32, greet, 0)

    gvec = gvec_ref[...]
    flat = gvec.astype(F32) + 0.5
    i = jnp.floor(flat * (1.0 / AREA)).astype(jnp.int32)
    ij = jnp.floor(flat * (1.0 / GRID)).astype(jnp.int32)
    group = jnp.floor((i.astype(F32) + 0.5) * (1.0 / 6)).astype(jnp.int32)
    lane = group * GRID + gvec - ij * GRID
    rid_ref[...] = ((i - group * 6) * 3 + (lane >> 7)) * GRID + ij - i * GRID
    lid_ref[...] = lane & 127

    valence = jnp.full((1, 256), ve_ref[bands_ref[0, n]], F32)
    conduction = jnp.full((1, 256), ce_ref[bands_ref[1, n]], F32)
    frequency = jnp.full((1, 256), freq_ref[0], F32)
    gap = conduction - valence
    weight = -4.0 * gap / (gap * gap + frequency * frequency) / math.sqrt(512.0)

    last = [jnp.concatenate([d4_ref[2 * q], d4_ref[2 * q + 1]], axis=0) for q in range(2)]
    dh, dl = hi_lo(jnp.concatenate([d8_ref[...].reshape(32, AREA), *last], axis=0))
    a = dot(cx_ref[...], jnp.concatenate([dh, dh, dl], axis=0))
    ah, al = hi_lo(a)
    third = AREA // 3
    lhs = jnp.concatenate(
        [half[:, b * third : (b + 1) * third] for half in (ah, al) for b in range(3)], axis=0
    )
    by_high = dot(lhs, bh_ref[...])
    by_low = dot(lhs[:192], bl_ref[...])
    for b in range(3):
        rows = slice(b * 64, (b + 1) * 64)
        z_ref[:, b * third : (b + 1) * third] = (
            by_high[rows] + by_high[192 + b * 64 : 256 + b * 64] + by_low[rows]
        )

    def relay(part, carry):
        lines = z_ref[:, pl.ds(pl.multiple_of(part * 384, 128), 384)]
        for y in range(8):
            s_ref[part * 8 + y] = jnp.concatenate(
                [lines[g * 8 : (g + 1) * 8, y * GRID : (y + 1) * GRID] for g in range(8)], axis=1
            )
        return carry

    lax.fori_loop(0, 6, relay, 0)
    for r in range(6):
        sh, sl = hi_lo(s_ref[:, r, :])
        t = dot(cy_ref[...], jnp.concatenate([sh, sh, sl], axis=0))
        for u in range(3):
            t_ref[(r * 3 + u) * GRID : (r * 3 + u + 1) * GRID, :] = t[:, u * 128 : (u + 1) * 128]
    th, tl = hi_lo(t_ref[...].T)
    tt_ref[0:128, :864] = th
    tt_ref[128:256, :864] = tl

    home = (z * CORES + c) * 32 + yh * 16 + me
    from_me = (z * CORES + c) * HIGH + yh

    def arrived(ref, sem):
        pltpu.make_async_copy(ref, ref, sem).wait()

    sends = []

    def send(src, dst, send_sem, recv_sem, **device):
        copy = pltpu.make_async_remote_copy(
            src_ref=src, dst_ref=dst, send_sem=send_sem, recv_sem=recv_sem, device_id=device, device_id_type=MESH
        )
        copy.start()
        sends.append(copy)

    for q in range(3):

        def chunk(k, carry, q=q):
            def pick(ref):
                return jnp.concatenate([ref[pl.ds(k * 6 + q, 1), :], ref[pl.ds(k * 6 + 3 + q, 1), :]], axis=1)

            rid, lid = pick(rid_ref), pick(lid_ref)
            acc = None
            for kt in range(4):
                kn = min(256, 864 - kt * 256)
                index = lax.broadcasted_iota(jnp.int32, (kn, 256), 0) + kt * 256
                hot = jnp.where(index == rid, 1.0, 0.0).astype(BF16)
                part = dot(tt_ref[:, kt * 256 : kt * 256 + kn], hot)
                acc = part if acc is None else acc + part
            both = acc[:128] + acc[128:]
            mine = lax.broadcasted_iota(jnp.int32, (128, 256), 0) == lid
            got = jnp.sum(jnp.where(mine, both, 0.0), axis=0, keepdims=True)
            heavy = got * weight
            row_ref[q * 16 + k, 0:1, :] = heavy[:, :128]
            row_ref[q * 16 + k, 1:2, :] = heavy[:, 128:]
            col_ref[q * 32 + 2 * k] = got[:, :128]
            col_ref[q * 32 + 2 * k + 1] = got[:, 128:]
            return carry

        lax.fori_loop(0, 16, chunk, 0)
        if q == 0:
            pl.semaphore_wait(barrier, 62)
        own_col = cols_ref.at[q * 512 + me * 32 + from_me]
        own_row = rows_ref.at[q * 512 + home]

        def spread(d, carry, q=q, own_row=own_row, own_col=own_col):
            sp, wp, np_ = row_peer(d)
            pltpu.make_async_remote_copy(
                src_ref=row_ref.at[q * 16 + sp * NARROW + np_], dst_ref=own_row, send_sem=send_small,
                recv_sem=recv_row1.at[q, d // 16],
                device_id={"section": sp, "wide": wp, "narrow": np_}, device_id_type=MESH,
            ).start()
            wc = col_peer(d)
            pltpu.make_async_remote_copy(
                src_ref=col_ref.at[q * 32 + wc], dst_ref=own_col, send_sem=send_small,
                recv_sem=recv_col1.at[q], device_id={"wide": wc}, device_id_type=MESH,
            ).start()
            return carry

        lax.fori_loop(1, 32, spread, 0)
        rows_ref[q * 512 + home] = row_ref[q * 16 + me]
        cols_ref[q * 512 + me * 32 + from_me] = col_ref[q * 32 + w]

    def sub(q, zz, cc, h):
        start = q * 512 + (zz * CORES + cc) * 32 + lax.rem(yh + h, HIGH) * 16
        return rows_ref.at[pl.ds(start, 16)]

    def ring_peer(step):
        return yh * (RING * CORES) + lax.rem(z + step + RING, RING) * CORES + c

    side = yh * (RING * CORES) + z * CORES + 1 - c

    def section_peer(step):
        return lax.rem(s + step + SECTION, SECTION)

    def cols_of(q, step, d):
        start = q * 512 + (section_peer(step) * NARROW + lax.rem(n - d + NARROW, NARROW)) * 32
        return cols_ref.at[pl.ds(start, 32)]

    ways = ((0, 1), (1, -1))

    def begin(q):
        mine = cols_of(q, 0, 0)
        arrived(cols_ref.at[pl.ds(q * 512, 31)], recv_col1.at[q])
        for d in range(1, NARROW):
            send(mine, mine, send_col, recv_y.at[q, d - 1], narrow=lax.rem(n + d, NARROW))
        for i, step in ways:
            send(mine, mine, send_col, recv_x.at[q, 0, i], section=section_peer(step))
        for h in range(2):
            arrived(rows_ref.at[pl.ds(q * 512, 15 + h)], recv_row1.at[q, h])
            block = sub(q, z, c, h)
            for i, step in ways:
                send(block, block, send_row, recv_ring.at[q, i, 0, h], wide=ring_peer(step))
            send(block, block, send_side, recv_side.at[q, 0, 0, h], wide=side)

    def ring_step(q, k):
        for h in range(2):
            for i, step in ways:
                if k == 4 and h != i:
                    continue
                got = sub(q, lax.rem(z - step * k + RING, RING), c, h)
                arrived(got, recv_ring.at[q, i, k - 1, h])
                if k < 3 or (k == 3 and h == i):
                    send(got, got, send_row, recv_ring.at[q, i, k, h], wide=ring_peer(step))
                send(got, got, send_side, recv_side.at[q, i, k, h], wide=side)

    def from_narrow(q, d):
        got = cols_of(q, 0, d)
        arrived(got, recv_y.at[q, d - 1])
        for i, step in ways:
            send(got, got, send_col, recv_x.at[q, d, i], section=section_peer(step))

    def along_section(q, d):
        i, step = ways[d % 2]
        got = cols_of(q, -step, d)
        arrived(got, recv_x.at[q, d, i])
        send(got, got, send_col, recv_xx.at[q, d], section=section_peer(step))

    def step(q, k):
        if k == 1:
            from_narrow(q, 1)
        elif k == 2:
            from_narrow(q, 3)
            from_narrow(q, 2)
            along_section(q, 0)
        elif k == 3:
            along_section(q, 1)
        ring_step(q, k)
        if k == 3:
            along_section(q, 3)
            along_section(q, 2)

    def finish(q):
        for d in range(NARROW):
            i, way = ways[1 - d % 2]
            arrived(cols_of(q, -way, d), recv_x.at[q, d, i])
            arrived(cols_of(q, 2, d), recv_xx.at[q, d])
        for h in range(2):
            arrived(sub(q, z, 1 - c, h), recv_side.at[q, 0, 0, h])
            for k in range(1, 5):
                for i, way in ways:
                    if k == 4 and h != i:
                        continue
                    arrived(sub(q, lax.rem(z - way * k + RING, RING), 1 - c, h), recv_side.at[q, i, k, h])
        lines = rows_ref.reshape(3072, 128)
        for half in range(2):
            left = lines[pl.ds(q * 1024 + half, 512, stride=2), :]
            lh, ll = hi_lo(left.T)
            here = slice(q * 256 + half * 128, q * 256 + half * 128 + 128)
            at_ref[here, 0:512] = lh
            at_ref[here, 512:1024] = lh
            at_ref[here, 1024:1536] = ll
        lines = cols_ref.reshape(1536, 128)
        right = jnp.concatenate(
            [lines[pl.ds(q * 512 + place, 16, stride=32), :] for place in range(32)], axis=0
        )
        rh, rl = hi_lo(right)
        here = slice(q * 128, q * 128 + 128)
        bb_ref[0:512, here] = rh
        bb_ref[512:1024, here] = rl
        bb_ref[1024:1536, here] = rh

    def multiply(q0, q1, c0, c1):
        part = dot(at_ref[q0 * 256 : q1 * 256, :], bb_ref[:, c0 * 128 : c1 * 128])
        for q in range(q0, q1):
            for half in range(2):
                first = (q - q0) * 256 + half * 128
                out_ref[half * 384 + q * 128 : half * 384 + q * 128 + 128, c0 * 128 : c1 * 128] = part[
                    first : first + 128
                ]

    begin(0)
    step(0, 1)
    begin(1)
    step(0, 2)
    step(1, 1)
    begin(2)
    step(0, 3)
    step(1, 2)
    step(2, 1)
    step(0, 4)
    step(1, 3)
    step(2, 2)
    step(1, 4)
    step(2, 3)
    finish(0)
    finish(1)
    multiply(0, 2, 0, 2)
    step(2, 4)
    finish(2)
    multiply(0, 2, 2, 3)
    multiply(2, 3, 0, 3)
    for copy in sends:
        copy.wait_send()
    for q in range(3):
        arrived(rows_ref.at[pl.ds(q * 512, 31)], send_small)
        arrived(cols_ref.at[pl.ds(q * 512, 31)], send_small)


def polarize(bands, ve, ce, freq, d8, d4, gvec):
    smem, vmem = pl.BlockSpec(memory_space=pltpu.SMEM), pl.BlockSpec(memory_space=pltpu.VMEM)
    dma = pltpu.SemaphoreType.DMA
    return pl.pallas_call(
        polarize_body,
        out_shape=jax.ShapeDtypeStruct((ROWS, COLS), F32),
        in_specs=[smem] * 4 + [vmem] * 7,
        out_specs=vmem,
        scratch_shapes=[
            pltpu.VMEM((96, 128), jnp.int32),
            pltpu.VMEM((96, 128), jnp.int32),
            pltpu.VMEM((64, AREA), F32),
            pltpu.VMEM((GRID, 8, 384), F32),
            pltpu.VMEM((864, 128), F32),
            pltpu.VMEM((256, 896), BF16),
            pltpu.VMEM((48, 2, 128), F32),
            pltpu.VMEM((96, 1, 128), F32),
            pltpu.VMEM((1536, 2, 128), F32),
            pltpu.VMEM((1536, 1, 128), F32),
            pltpu.VMEM((ROWS, 1536), BF16),
            pltpu.VMEM((1536, COLS), BF16),
            dma, dma, dma, dma,
            dma((3, 2)), dma((3,)), dma((3, 2, 4, 2)), dma((3, 2, 5, 2)), dma((3, 3)), dma((3, 4, 2)), dma((3, 4)),
        ],
        compiler_params=pltpu.CompilerParams(
            collective_id=1, has_side_effects=True, vmem_limit_bytes=40 * 1024 * 1024
        ),
        name="polarize",
    )(bands, ve, ce, freq, d8, d4, gvec, *[jnp.asarray(t) for t in tables()])


def on_device(ve_orb, ce_orb, ve, ce, freq, bands, gvec):
    tiles = AREA // 128
    valence = ve_orb.reshape(8, PLANES, tiles, 128).transpose(1, 2, 0, 3).reshape(-1, 128)
    conduction = ce_orb.reshape(PLANES * tiles, 128)
    d8, d4 = exchange(bands.T, valence, conduction)
    return polarize(bands.T, ve, ce, freq, d8, d4, gvec.reshape(96, 128))


def solution(mesh):
    in_specs = (
        P(None, "narrow", None),
        P(("section", "wide"), "narrow", None),
        P(),
        P(),
        P(),
        P(("section", "wide"), None),
        P(),
    )
    return jax.shard_map(
        on_device,
        mesh=mesh,
        in_specs=in_specs,
        out_specs=P(("section", "narrow"), "wide"),
        check_vma=False,
    )
```

```python
import functools
import math

import jax
import jax.numpy as jnp
import numpy as np
from jax import lax
from jax.experimental import pallas as pl
from jax.experimental.pallas import tpu as pltpu
from jax.sharding import PartitionSpec as P

F32, BF16 = jnp.float32, jnp.bfloat16
MESH = pl.DeviceIdType.MESH
GRID, NARROW, SECTION = 48, 4, 4
HIGH, RING, CORES = 2, 8, 2
WIDE = HIGH * RING * CORES
PLANES = GRID // NARROW
AREA = GRID * GRID
VECTORS = 12288
ROWS, COLS = VECTORS // 16, VECTORS // 32


def split_np(a):
    a = np.asarray(a, np.float32)
    h = a.astype(BF16)
    return h, (a - h.astype(np.float32)).astype(BF16)


def tables():
    k, x = np.arange(GRID)[:, None], np.arange(GRID)[None, :]
    c = math.sqrt(2.0 / GRID) * np.cos(math.pi * (2 * x + 1) * k / (2 * GRID))
    c[0] *= math.sqrt(0.5)
    cx = np.zeros((64, GRID))
    order = [p * PLANES + q for p in range(4) for q in range(8)] + [p * PLANES + q for p in range(4) for q in range(8, 12)]
    for i in range(GRID):
        cx[(i // 6) * 8 + i % 6] = c[i, order]
    h, l = split_np(cx)
    cx3 = np.concatenate([h, l, h], axis=1)
    bh, bl = split_np(np.kron(np.eye(8), c.T))
    h, l = split_np(c)
    cy3 = np.concatenate([h, l, h], axis=1)
    return cx3, bh, bl, cy3


def hi_lo(a):
    h = a.astype(BF16)
    return h, (a - h.astype(F32)).astype(BF16)


def dot(a, b):
    return lax.dot_general(a, b, (((1,), (0,)), ((), ())), preferred_element_type=F32)


def exchange_body(
    bands_hbm, valence_hbm, conduction_hbm, bh_hbm, bl_hbm, cx_hbm,
    s_ref,
    bands_ref, valence_ref, conduction_ref, bh_ref, bl_ref, cx_ref, stage8_ref, stage4_ref, d8_ref, d4_ref, z_ref, load_sem, send_sem, recv_sem,
):
    me = lax.axis_index("narrow")
    barrier = pltpu.get_barrier_semaphore()
    for d in range(1, NARROW):
        pl.semaphore_signal(
            barrier, inc=1, device_id={"narrow": lax.rem(me + d, NARROW)}, device_id_type=MESH
        )
    loads = [
        pltpu.make_async_copy(src, dst, load_sem.at[i])
        for i, (src, dst) in enumerate(
            (
                (bands_hbm, bands_ref),
                (conduction_hbm, conduction_ref),
                (valence_hbm, valence_ref),
                (cx_hbm, cx_ref),
                (bh_hbm, bh_ref),
                (bl_hbm, bl_ref),
            )
        )
    ]
    for load in loads:
        load.start()
    for load in loads[:3]:
        load.wait()
    for t in range(AREA // 128):
        conduction = conduction_ref[pl.ds(t, PLANES, stride=AREA // 128), :]
        lanes = slice(t * 128, (t + 1) * 128)
        for p in range(NARROW):
            valence = valence_ref[pl.ds(t * 8 + bands_ref[0, p], PLANES, stride=AREA // 16), :]
            density = valence * conduction
            stage8_ref[p, :, lanes] = density[:8]
            stage4_ref[p, :, lanes] = density[8:]
    pl.semaphore_wait(barrier, NARROW - 1)
    third = AREA // 3
    copies = []
    for b in range(3):
        lanes = slice(b * third, (b + 1) * third)
        for d in range(1, NARROW):
            peer = lax.rem(me + d, NARROW)
            for part, (src, dst) in enumerate(((stage8_ref, d8_ref), (stage4_ref, d4_ref))):
                copy = pltpu.make_async_remote_copy(
                    src_ref=src.at[peer, :, lanes],
                    dst_ref=dst.at[me, :, lanes],
                    send_sem=send_sem.at[b, part, d - 1],
                    recv_sem=recv_sem.at[b, part, d - 1],
                    device_id={"narrow": peer},
                    device_id_type=MESH,
                )
                copy.start()
                copies.append(copy)
    d8_ref[me] = stage8_ref[me]
    d4_ref[me] = stage4_ref[me]
    for load in loads[3:]:
        load.wait()
    per_third = len(copies) // 3
    for b in range(3):
        for copy in copies[b * per_third : (b + 1) * per_third]:
            copy.wait_recv()
        lanes = slice(b * third, (b + 1) * third)
        planes = [d8_ref[q, :, lanes] for q in range(NARROW)]
        planes += [
            jnp.concatenate([d4_ref[2 * q, :, lanes], d4_ref[2 * q + 1, :, lanes]], axis=0) for q in range(2)
        ]
        dh, dl = hi_lo(jnp.concatenate(planes, axis=0))
        a = dot(cx_ref[...], jnp.concatenate([dh, dh, dl], axis=0))
        ah, al = hi_lo(a)
        lhs = jnp.concatenate([ah[:, :384], ah[:, 384:], al[:, :384], al[:, 384:]], axis=0)
        by_high = dot(lhs, bh_ref[...])
        by_low = dot(lhs[:128], bl_ref[...])
        z_ref[...] = by_high[:128] + by_high[128:] + by_low

        def relay(half, carry, b=b):
            lines = z_ref[pl.ds(pl.multiple_of(half * 64, 64), 64), :]
            for y in range(8):
                s_ref[b * 16 + half * 8 + y] = jnp.concatenate(
                    [lines[g * 8 : (g + 1) * 8, y * GRID : (y + 1) * GRID] for g in range(8)], axis=1
                )
            return carry

        lax.fori_loop(0, 2, relay, 0)
    for copy in copies:
        copy.wait_send()


def exchange(bands, valence, conduction, cx3, bh, bl):
    vmem, hbm = pl.BlockSpec(memory_space=pltpu.VMEM), pl.BlockSpec(memory_space=pltpu.HBM)
    return pl.pallas_call(
        exchange_body,
        out_shape=jax.ShapeDtypeStruct((GRID, 8, 384), F32),
        in_specs=[hbm] * 6,
        out_specs=vmem,
        scratch_shapes=[
            pltpu.SMEM((2, NARROW), jnp.int32),
            pltpu.VMEM(valence.shape, F32),
            pltpu.VMEM(conduction.shape, F32),
            pltpu.VMEM((384, 384), BF16),
            pltpu.VMEM((384, 384), BF16),
            pltpu.VMEM(cx3.shape, BF16),
            pltpu.VMEM((NARROW, 8, AREA), F32),
            pltpu.VMEM((NARROW, 4, AREA), F32),
            pltpu.VMEM((NARROW, 8, AREA), F32),
            pltpu.VMEM((NARROW, 4, AREA), F32),
            pltpu.VMEM((128, 384), F32),
            pltpu.SemaphoreType.DMA((6,)),
            pltpu.SemaphoreType.DMA((3, 2, NARROW - 1)),
            pltpu.SemaphoreType.DMA((3, 2, NARROW - 1)),
        ],
        compiler_params=pltpu.CompilerParams(
            collective_id=0, has_side_effects=True, vmem_limit_bytes=16 * 1024 * 1024
        ),
        cost_estimate=pl.CostEstimate(flops=10**10, bytes_accessed=2 * 10**7, transcendentals=0),
        name="exchange",
    )(*(pltpu.with_memory_space_constraint(a, pltpu.HBM) for a in (bands, valence, conduction, bh, bl, cx3)))


def polarize_body(
    bands_ref, ve_ref, ce_ref, freq_ref, s_ref, gvec_ref, cy_ref,
    out_ref,
    rid_ref, lid_ref, t_ref, tt_ref, row_ref, col_ref, rows_ref, cols_ref, at_ref, bb_ref,
    send_small, send_row, send_side, send_col,
    recv_row1, recv_col1, recv_ring, recv_side, recv_y, recv_x, recv_xx,
):
    s, w, n = lax.axis_index("section"), lax.axis_index("wide"), lax.axis_index("narrow")
    yh, z, c = w // (RING * CORES), lax.rem(w // CORES, RING), lax.rem(w, CORES)
    me = s * NARROW + n

    def row_peer(d):
        sp, np_ = lax.rem(s + lax.rem(d, 4), SECTION), lax.rem(n + lax.rem(d // 4, 4), NARROW)
        wp = lax.rem(yh + d // 16, HIGH) * (RING * CORES) + z * CORES + c
        return sp, wp, np_

    def col_peer(d):
        return lax.rem(w + d, WIDE)

    barrier = pltpu.get_barrier_semaphore()

    def greet(d, carry):
        sp, wp, np_ = row_peer(d)
        pl.semaphore_signal(
            barrier, inc=1, device_id={"section": sp, "wide": wp, "narrow": np_}, device_id_type=MESH
        )
        pl.semaphore_signal(barrier, inc=1, device_id={"wide": col_peer(d)}, device_id_type=MESH)
        return carry

    lax.fori_loop(1, 32, greet, 0)

    gvec = gvec_ref[...]
    flat = gvec.astype(F32) + 0.5
    i = jnp.floor(flat * (1.0 / AREA)).astype(jnp.int32)
    ij = jnp.floor(flat * (1.0 / GRID)).astype(jnp.int32)
    group = jnp.floor((i.astype(F32) + 0.5) * (1.0 / 6)).astype(jnp.int32)
    lane = group * GRID + gvec - ij * GRID
    rid_ref[...] = ((i - group * 6) * 3 + (lane >> 7)) * GRID + ij - i * GRID
    lid_ref[...] = lane & 127

    valence = jnp.full((1, 256), ve_ref[bands_ref[0, n]], F32)
    conduction = jnp.full((1, 256), ce_ref[bands_ref[1, n]], F32)
    frequency = jnp.full((1, 256), freq_ref[0], F32)
    gap = conduction - valence
    weight = -4.0 * gap / (gap * gap + frequency * frequency) / math.sqrt(512.0)

    for r in range(6):
        sh, sl = hi_lo(s_ref[:, r, :])
        t = dot(cy_ref[...], jnp.concatenate([sh, sh, sl], axis=0))
        for u in range(3):
            t_ref[(r * 3 + u) * GRID : (r * 3 + u + 1) * GRID, :] = t[:, u * 128 : (u + 1) * 128]
    th, tl = hi_lo(t_ref[...].T)
    tt_ref[0:128, :864] = th
    tt_ref[128:256, :864] = tl

    home = (z * CORES + c) * 32 + yh * 16 + me
    from_me = (z * CORES + c) * HIGH + yh

    def arrived(ref, sem):
        pltpu.make_async_copy(ref, ref, sem).wait()

    sends = []

    def send(src, dst, send_sem, recv_sem, **device):
        copy = pltpu.make_async_remote_copy(
            src_ref=src, dst_ref=dst, send_sem=send_sem, recv_sem=recv_sem, device_id=device, device_id_type=MESH
        )
        copy.start()
        sends.append(copy)

    for q in range(3):

        def chunk(k, q=q):
            def pick(ref):
                return jnp.concatenate([ref[pl.ds(k * 6 + q, 1), :], ref[pl.ds(k * 6 + 3 + q, 1), :]], axis=1)

            rid, lid = pick(rid_ref), pick(lid_ref)
            acc = None
            for kt in range(4):
                kn = min(256, 864 - kt * 256)
                index = lax.broadcasted_iota(jnp.int32, (kn, 256), 0) + kt * 256
                hot = jnp.where(index == rid, 1.0, 0.0).astype(BF16)
                part = dot(tt_ref[:, kt * 256 : kt * 256 + kn], hot)
                acc = part if acc is None else acc + part
            both = acc[:128] + acc[128:]
            mine = lax.broadcasted_iota(jnp.int32, (128, 256), 0) == lid
            got = jnp.sum(jnp.where(mine, both, 0.0), axis=0, keepdims=True)
            heavy = got * weight
            row_ref[q * 16 + k, 0:1, :] = heavy[:, :128]
            row_ref[q * 16 + k, 1:2, :] = heavy[:, 128:]
            col_ref[q * 32 + 2 * k] = got[:, :128]
            col_ref[q * 32 + 2 * k + 1] = got[:, 128:]

        def chunks(group, carry, chunk=chunk):
            for k in range(8):
                chunk(group * 8 + k)
            return carry

        lax.fori_loop(0, 2, chunks, 0)
        if q == 0:
            pl.semaphore_wait(barrier, 62)
        own_col = cols_ref.at[q * 512 + me * 32 + from_me]
        own_row = rows_ref.at[q * 512 + home]

        def spread(d, carry, q=q, own_row=own_row, own_col=own_col):
            sp, wp, np_ = row_peer(d)
            pltpu.make_async_remote_copy(
                src_ref=row_ref.at[q * 16 + sp * NARROW + np_], dst_ref=own_row, send_sem=send_small,
                recv_sem=recv_row1.at[q, d // 16],
                device_id={"section": sp, "wide": wp, "narrow": np_}, device_id_type=MESH,
            ).start()
            wc = col_peer(d)
            pltpu.make_async_remote_copy(
                src_ref=col_ref.at[q * 32 + wc], dst_ref=own_col, send_sem=send_small,
                recv_sem=recv_col1.at[q], device_id={"wide": wc}, device_id_type=MESH,
            ).start()
            return carry

        lax.fori_loop(1, 32, spread, 0)
        rows_ref[q * 512 + home] = row_ref[q * 16 + me]
        cols_ref[q * 512 + me * 32 + from_me] = col_ref[q * 32 + w]

    def sub(q, zz, cc, h):
        start = q * 512 + (zz * CORES + cc) * 32 + lax.rem(yh + h, HIGH) * 16
        return rows_ref.at[pl.ds(start, 16)]

    def ring_peer(step):
        return yh * (RING * CORES) + lax.rem(z + step + RING, RING) * CORES + c

    side = yh * (RING * CORES) + z * CORES + 1 - c

    def section_peer(step):
        return lax.rem(s + step + SECTION, SECTION)

    def cols_of(q, step, d):
        start = q * 512 + (section_peer(step) * NARROW + lax.rem(n - d + NARROW, NARROW)) * 32
        return cols_ref.at[pl.ds(start, 32)]

    ways = ((0, 1), (1, -1))

    def begin(q):
        mine = cols_of(q, 0, 0)
        arrived(cols_ref.at[pl.ds(q * 512, 31)], recv_col1.at[q])
        for d in range(1, NARROW):
            send(mine, mine, send_col, recv_y.at[q, d - 1], narrow=lax.rem(n + d, NARROW))
        for i, step in ways:
            send(mine, mine, send_col, recv_x.at[q, 0, i], section=section_peer(step))
        for h in range(2):
            arrived(rows_ref.at[pl.ds(q * 512, 15 + h)], recv_row1.at[q, h])
            block = sub(q, z, c, h)
            for i, step in ways:
                if q < 2:
                    send(block, block, send_row, recv_ring.at[q, i, 0, h], wide=ring_peer(step))
                    continue
                for k in (4, 3, 2, 1):
                    if k < 4 or h == i:
                        send(block, block, send_row, recv_ring.at[q, i, k - 1, h], wide=ring_peer(step * k))
            send(block, block, send_side, recv_side.at[q, 0, 0, h], wide=side)

    def ring_step(q, k):
        for h in range(2):
            for i, step in ways:
                if k == 4 and h != i:
                    continue
                got = sub(q, lax.rem(z - step * k + RING, RING), c, h)
                arrived(got, recv_ring.at[q, i, k - 1, h])
                if q < 2 and (k < 3 or (k == 3 and h == i)):
                    send(got, got, send_row, recv_ring.at[q, i, k, h], wide=ring_peer(step))
                send(got, got, send_side, recv_side.at[q, i, k, h], wide=side)

    def from_narrow(q, d):
        got = cols_of(q, 0, d)
        arrived(got, recv_y.at[q, d - 1])
        for i, step in ways:
            send(got, got, send_col, recv_x.at[q, d, i], section=section_peer(step))

    def along_section(q, d):
        i, step = ways[d % 2]
        got = cols_of(q, -step, d)
        arrived(got, recv_x.at[q, d, i])
        send(got, got, send_col, recv_xx.at[q, d], section=section_peer(step))

    def step(q, k):
        if k == 1:
            from_narrow(q, 1)
        elif k == 2:
            from_narrow(q, 3)
            from_narrow(q, 2)
            along_section(q, 0)
        elif k == 3:
            along_section(q, 1)
        ring_step(q, k)
        if k == 3:
            along_section(q, 3)
            along_section(q, 2)

    def finish(q):
        for d in range(NARROW):
            i, way = ways[1 - d % 2]
            arrived(cols_of(q, -way, d), recv_x.at[q, d, i])
            arrived(cols_of(q, 2, d), recv_xx.at[q, d])
        for h in range(2):
            arrived(sub(q, z, 1 - c, h), recv_side.at[q, 0, 0, h])
            for k in range(1, 5):
                for i, way in ways:
                    if k == 4 and h != i:
                        continue
                    arrived(sub(q, lax.rem(z - way * k + RING, RING), 1 - c, h), recv_side.at[q, i, k, h])
        lines = rows_ref.reshape(3072, 128)
        for half in range(2):
            left = lines[pl.ds(q * 1024 + half, 512, stride=2), :]
            lh, ll = hi_lo(left.T)
            here = slice(q * 256 + half * 128, q * 256 + half * 128 + 128)
            at_ref[here, 0:512] = lh
            at_ref[here, 512:1024] = lh
            at_ref[here, 1024:1536] = ll
        lines = cols_ref.reshape(1536, 128)
        right = jnp.concatenate(
            [lines[pl.ds(q * 512 + place, 16, stride=32), :] for place in range(32)], axis=0
        )
        rh, rl = hi_lo(right)
        here = slice(q * 128, q * 128 + 128)
        bb_ref[0:512, here] = rh
        bb_ref[512:1024, here] = rl
        bb_ref[1024:1536, here] = rh

    def multiply(q0, q1, c0, c1):
        part = dot(at_ref[q0 * 256 : q1 * 256, :], bb_ref[:, c0 * 128 : c1 * 128])
        for q in range(q0, q1):
            for half in range(2):
                first = (q - q0) * 256 + half * 128
                out_ref[half * 384 + q * 128 : half * 384 + q * 128 + 128, c0 * 128 : c1 * 128] = part[
                    first : first + 128
                ]

    begin(0)
    step(0, 1)
    begin(1)
    step(0, 2)
    step(1, 1)
    begin(2)
    step(0, 3)
    step(1, 2)
    step(2, 1)
    step(0, 4)
    step(1, 3)
    step(2, 2)
    step(1, 4)
    step(2, 3)
    finish(0)
    finish(1)
    multiply(0, 2, 0, 2)
    step(2, 4)
    finish(2)
    multiply(0, 2, 2, 3)
    multiply(2, 3, 0, 3)
    for copy in sends:
        copy.wait_send()
    for q in range(3):
        arrived(rows_ref.at[pl.ds(q * 512, 31)], send_small)
        arrived(cols_ref.at[pl.ds(q * 512, 31)], send_small)


def polarize(bands, ve, ce, freq, lines, gvec, cy3):
    smem, vmem = pl.BlockSpec(memory_space=pltpu.SMEM), pl.BlockSpec(memory_space=pltpu.VMEM)
    dma = pltpu.SemaphoreType.DMA
    return pl.pallas_call(
        polarize_body,
        out_shape=jax.ShapeDtypeStruct((ROWS, COLS), F32),
        in_specs=[smem] * 4 + [vmem] * 3,
        out_specs=vmem,
        scratch_shapes=[
            pltpu.VMEM((96, 128), jnp.int32),
            pltpu.VMEM((96, 128), jnp.int32),
            pltpu.VMEM((864, 128), F32),
            pltpu.VMEM((256, 896), BF16),
            pltpu.VMEM((48, 2, 128), F32),
            pltpu.VMEM((96, 1, 128), F32),
            pltpu.VMEM((1536, 2, 128), F32),
            pltpu.VMEM((1536, 1, 128), F32),
            pltpu.VMEM((ROWS, 1536), BF16),
            pltpu.VMEM((1536, COLS), BF16),
            dma, dma, dma, dma,
            dma((3, 2)), dma((3,)), dma((3, 2, 4, 2)), dma((3, 2, 5, 2)), dma((3, 3)), dma((3, 4, 2)), dma((3, 4)),
        ],
        compiler_params=pltpu.CompilerParams(
            collective_id=1, has_side_effects=True, vmem_limit_bytes=40 * 1024 * 1024
        ),
        name="polarize",
    )(bands, ve, ce, freq, lines, gvec, cy3)


def on_device(ve_orb, ce_orb, ve, ce, freq, bands, gvec):
    tiles = AREA // 128
    valence = ve_orb.reshape(8, PLANES, tiles, 128).transpose(1, 2, 0, 3).reshape(-1, 128)
    conduction = ce_orb.reshape(PLANES * tiles, 128)
    cx3, bh, bl, cy3 = (jnp.asarray(t) for t in tables())
    lines = exchange(bands.T, valence, conduction, cx3, bh, bl)
    return polarize(bands.T, ve, ce, freq, lines, gvec.reshape(96, 128), cy3)


def solution(mesh):
    in_specs = (
        P(None, "narrow", None),
        P(("section", "wide"), "narrow", None),
        P(),
        P(),
        P(),
        P(("section", "wide"), None),
        P(),
    )
    return jax.shard_map(
        on_device,
        mesh=mesh,
        in_specs=in_specs,
        out_specs=P(("section", "narrow"), "wide"),
        check_vma=False,
    )
```

```python
import functools
import math

import jax
import jax.numpy as jnp
import numpy as np
from jax import lax
from jax.experimental import pallas as pl
from jax.experimental.pallas import tpu as pltpu
from jax.sharding import PartitionSpec as P

F32, BF16 = jnp.float32, jnp.bfloat16
MESH = pl.DeviceIdType.MESH
GRID, NARROW, SECTION = 48, 4, 4
HIGH, RING, CORES = 2, 8, 2
WIDE = HIGH * RING * CORES
PLANES = GRID // NARROW
AREA = GRID * GRID
VECTORS = 12288
ROWS, COLS = VECTORS // 16, VECTORS // 32


def split_np(a):
    a = np.asarray(a, np.float32)
    h = a.astype(BF16)
    return h, (a - h.astype(np.float32)).astype(BF16)


def tables():
    k, x = np.arange(GRID)[:, None], np.arange(GRID)[None, :]
    c = math.sqrt(2.0 / GRID) * np.cos(math.pi * (2 * x + 1) * k / (2 * GRID))
    c[0] *= math.sqrt(0.5)
    cx = np.zeros((64, GRID))
    order = [p * PLANES + q for p in range(4) for q in range(8)] + [p * PLANES + q for p in range(4) for q in range(8, 12)]
    for i in range(GRID):
        cx[(i // 6) * 8 + i % 6] = c[i, order]
    h, l = split_np(cx)
    cx3 = np.concatenate([h, l, h], axis=1)
    bh, bl = split_np(np.kron(np.eye(8), c.T))
    h, l = split_np(c)
    cy3 = np.concatenate([h, l, h], axis=1)
    return cx3, bh, bl, cy3


def hi_lo(a):
    h = a.astype(BF16)
    return h, (a - h.astype(F32)).astype(BF16)


def dot(a, b):
    return lax.dot_general(a, b, (((1,), (0,)), ((), ())), preferred_element_type=F32)


def exchange_body(
    bands_hbm, valence_hbm, conduction_hbm, bh_hbm, bl_hbm, cx_hbm,
    s_ref,
    bands_ref, valence_ref, conduction_ref, bh_ref, bl_ref, cx_ref, stage8_ref, stage4_ref, d8_ref, d4_ref, z_ref, load_sem, send_sem, recv_sem,
):
    me = lax.axis_index("narrow")
    barrier = pltpu.get_barrier_semaphore()
    for d in range(1, NARROW):
        pl.semaphore_signal(
            barrier, inc=1, device_id={"narrow": lax.rem(me + d, NARROW)}, device_id_type=MESH
        )
    loads = [
        pltpu.make_async_copy(src, dst, load_sem.at[i])
        for i, (src, dst) in enumerate(
            (
                (bands_hbm, bands_ref),
                (conduction_hbm, conduction_ref),
                (valence_hbm, valence_ref),
                (cx_hbm, cx_ref),
                (bh_hbm, bh_ref),
                (bl_hbm, bl_ref),
            )
        )
    ]
    for load in loads:
        load.start()
    for load in loads[:3]:
        load.wait()
    for t in range(AREA // 128):
        conduction = conduction_ref[pl.ds(t, PLANES, stride=AREA // 128), :]
        lanes = slice(t * 128, (t + 1) * 128)
        for p in range(NARROW):
            valence = valence_ref[pl.ds(t * 8 + bands_ref[0, p], PLANES, stride=AREA // 16), :]
            density = valence * conduction
            stage8_ref[p, :, lanes] = density[:8]
            stage4_ref[p, :, lanes] = density[8:]
    pl.semaphore_wait(barrier, NARROW - 1)
    third = AREA // 3
    copies = []
    for b in range(3):
        lanes = slice(b * third, (b + 1) * third)
        for d in range(1, NARROW):
            peer = lax.rem(me + d, NARROW)
            for part, (src, dst) in enumerate(((stage8_ref, d8_ref), (stage4_ref, d4_ref))):
                copy = pltpu.make_async_remote_copy(
                    src_ref=src.at[peer, :, lanes],
                    dst_ref=dst.at[me, :, lanes],
                    send_sem=send_sem.at[b, part, d - 1],
                    recv_sem=recv_sem.at[b, part, d - 1],
                    device_id={"narrow": peer},
                    device_id_type=MESH,
                )
                copy.start()
                copies.append(copy)
    d8_ref[me] = stage8_ref[me]
    d4_ref[me] = stage4_ref[me]
    for load in loads[3:]:
        load.wait()
    per_third = len(copies) // 3
    for b in range(3):
        for copy in copies[b * per_third : (b + 1) * per_third]:
            copy.wait_recv()
        lanes = slice(b * third, (b + 1) * third)
        planes = [d8_ref[q, :, lanes] for q in range(NARROW)]
        planes += [
            jnp.concatenate([d4_ref[2 * q, :, lanes], d4_ref[2 * q + 1, :, lanes]], axis=0) for q in range(2)
        ]
        dh, dl = hi_lo(jnp.concatenate(planes, axis=0))
        a = dot(cx_ref[...], jnp.concatenate([dh, dh, dl], axis=0))
        ah, al = hi_lo(a)
        lhs = jnp.concatenate([ah[:, :384], ah[:, 384:], al[:, :384], al[:, 384:]], axis=0)
        by_high = dot(lhs, bh_ref[...])
        by_low = dot(lhs[:128], bl_ref[...])
        z_ref[...] = by_high[:128] + by_high[128:] + by_low

        def relay(half, carry, b=b):
            lines = z_ref[pl.ds(pl.multiple_of(half * 64, 64), 64), :]
            for y in range(8):
                s_ref[b * 16 + half * 8 + y] = jnp.concatenate(
                    [lines[g * 8 : (g + 1) * 8, y * GRID : (y + 1) * GRID] for g in range(8)], axis=1
                )
            return carry

        lax.fori_loop(0, 2, relay, 0)
    for copy in copies:
        copy.wait_send()


def exchange(bands, valence, conduction, cx3, bh, bl):
    vmem, hbm = pl.BlockSpec(memory_space=pltpu.VMEM), pl.BlockSpec(memory_space=pltpu.HBM)
    return pl.pallas_call(
        exchange_body,
        out_shape=jax.ShapeDtypeStruct((GRID, 8, 384), F32),
        in_specs=[hbm] * 6,
        out_specs=vmem,
        scratch_shapes=[
            pltpu.SMEM((2, NARROW), jnp.int32),
            pltpu.VMEM(valence.shape, F32),
            pltpu.VMEM(conduction.shape, F32),
            pltpu.VMEM((384, 384), BF16),
            pltpu.VMEM((384, 384), BF16),
            pltpu.VMEM(cx3.shape, BF16),
            pltpu.VMEM((NARROW, 8, AREA), F32),
            pltpu.VMEM((NARROW, 4, AREA), F32),
            pltpu.VMEM((NARROW, 8, AREA), F32),
            pltpu.VMEM((NARROW, 4, AREA), F32),
            pltpu.VMEM((128, 384), F32),
            pltpu.SemaphoreType.DMA((6,)),
            pltpu.SemaphoreType.DMA((3, 2, NARROW - 1)),
            pltpu.SemaphoreType.DMA((3, 2, NARROW - 1)),
        ],
        compiler_params=pltpu.CompilerParams(
            collective_id=0, has_side_effects=True, vmem_limit_bytes=16 * 1024 * 1024
        ),
        cost_estimate=pl.CostEstimate(flops=10**10, bytes_accessed=2 * 10**7, transcendentals=0),
        name="exchange",
    )(*(pltpu.with_memory_space_constraint(a, pltpu.HBM) for a in (bands, valence, conduction, bh, bl, cx3)))


def polarize_body(
    bands_ref, ve_ref, ce_ref, freq_ref, s_ref, gvec_ref, cy_ref,
    out_ref,
    rid_ref, lid_ref, t_ref, tt_ref, row_ref, col_ref, rows_ref, cols_ref, at_ref, bb_ref,
    send_small, send_row, send_side, send_col,
    recv_row1, recv_col1, recv_ring, recv_side, recv_y, recv_x, recv_xx,
):
    s, w, n = lax.axis_index("section"), lax.axis_index("wide"), lax.axis_index("narrow")
    yh, z, c = w // (RING * CORES), lax.rem(w // CORES, RING), lax.rem(w, CORES)
    me = s * NARROW + n

    def row_peer(d):
        sp, np_ = lax.rem(s + lax.rem(d, 4), SECTION), lax.rem(n + lax.rem(d // 4, 4), NARROW)
        wp = lax.rem(yh + d // 16, HIGH) * (RING * CORES) + z * CORES + c
        return sp, wp, np_

    def col_peer(d):
        return lax.rem(w + d, WIDE)

    barrier = pltpu.get_barrier_semaphore()

    def greet(d, carry):
        sp, wp, np_ = row_peer(d)
        pl.semaphore_signal(
            barrier, inc=1, device_id={"section": sp, "wide": wp, "narrow": np_}, device_id_type=MESH
        )
        pl.semaphore_signal(barrier, inc=1, device_id={"wide": col_peer(d)}, device_id_type=MESH)
        return carry

    lax.fori_loop(1, 32, greet, 0)

    gvec = gvec_ref[...]
    flat = gvec.astype(F32) + 0.5
    i = jnp.floor(flat * (1.0 / AREA)).astype(jnp.int32)
    ij = jnp.floor(flat * (1.0 / GRID)).astype(jnp.int32)
    group = jnp.floor((i.astype(F32) + 0.5) * (1.0 / 6)).astype(jnp.int32)
    lane = group * GRID + gvec - ij * GRID
    rid_ref[...] = ((i - group * 6) * 3 + (lane >> 7)) * GRID + ij - i * GRID
    lid_ref[...] = lane & 127

    valence = jnp.full((1, 256), ve_ref[bands_ref[0, n]], F32)
    conduction = jnp.full((1, 256), ce_ref[bands_ref[1, n]], F32)
    frequency = jnp.full((1, 256), freq_ref[0], F32)
    gap = conduction - valence
    weight = -4.0 * gap / (gap * gap + frequency * frequency) / math.sqrt(512.0)

    for r in range(6):
        sh, sl = hi_lo(s_ref[:, r, :])
        t = dot(cy_ref[...], jnp.concatenate([sh, sh, sl], axis=0))
        for u in range(3):
            t_ref[(r * 3 + u) * GRID : (r * 3 + u + 1) * GRID, :] = t[:, u * 128 : (u + 1) * 128]
    th, tl = hi_lo(t_ref[...].T)
    tt_ref[0:128, :864] = th
    tt_ref[128:256, :864] = tl

    home = (z * CORES + c) * 32 + yh * 16 + me
    from_me = (z * CORES + c) * HIGH + yh

    def arrived(ref, sem):
        pltpu.make_async_copy(ref, ref, sem).wait()

    sends = []

    def send(src, dst, send_sem, recv_sem, **device):
        copy = pltpu.make_async_remote_copy(
            src_ref=src, dst_ref=dst, send_sem=send_sem, recv_sem=recv_sem, device_id=device, device_id_type=MESH
        )
        copy.start()
        sends.append(copy)

    for q in range(3):

        def chunk(k, q=q):
            def pick(ref):
                return jnp.concatenate([ref[pl.ds(k * 6 + q, 1), :], ref[pl.ds(k * 6 + 3 + q, 1), :]], axis=1)

            rid, lid = pick(rid_ref), pick(lid_ref)
            acc = None
            for kt in range(4):
                kn = min(256, 864 - kt * 256)
                index = lax.broadcasted_iota(jnp.int32, (kn, 256), 0) + kt * 256
                hot = jnp.where(index == rid, 1.0, 0.0).astype(BF16)
                part = dot(tt_ref[:, kt * 256 : kt * 256 + kn], hot)
                acc = part if acc is None else acc + part
            both = acc[:128] + acc[128:]
            mine = lax.broadcasted_iota(jnp.int32, (128, 256), 0) == lid
            got = jnp.sum(jnp.where(mine, both, 0.0), axis=0, keepdims=True)
            heavy = got * weight
            row_ref[q * 16 + k, 0:1, :] = heavy[:, :128]
            row_ref[q * 16 + k, 1:2, :] = heavy[:, 128:]
            col_ref[q * 32 + 2 * k] = got[:, :128]
            col_ref[q * 32 + 2 * k + 1] = got[:, 128:]

        def chunks(group, carry, chunk=chunk):
            for k in range(8):
                chunk(group * 8 + k)
            return carry

        lax.fori_loop(0, 2, chunks, 0)
        if q == 0:
            pl.semaphore_wait(barrier, 62)
        own_col = cols_ref.at[q * 512 + me * 32 + from_me]
        own_row = rows_ref.at[q * 512 + home]

        def spread(d, carry, q=q, own_row=own_row, own_col=own_col):
            sp, wp, np_ = row_peer(d)
            pltpu.make_async_remote_copy(
                src_ref=row_ref.at[q * 16 + sp * NARROW + np_], dst_ref=own_row, send_sem=send_small,
                recv_sem=recv_row1.at[q, d // 16],
                device_id={"section": sp, "wide": wp, "narrow": np_}, device_id_type=MESH,
            ).start()
            wc = col_peer(d)
            pltpu.make_async_remote_copy(
                src_ref=col_ref.at[q * 32 + wc], dst_ref=own_col, send_sem=send_small,
                recv_sem=recv_col1.at[q], device_id={"wide": wc}, device_id_type=MESH,
            ).start()
            return carry

        lax.fori_loop(1, 32, spread, 0)
        rows_ref[q * 512 + home] = row_ref[q * 16 + me]
        cols_ref[q * 512 + me * 32 + from_me] = col_ref[q * 32 + w]

    def sub(q, zz, cc, h):
        start = q * 512 + (zz * CORES + cc) * 32 + lax.rem(yh + h, HIGH) * 16
        return rows_ref.at[pl.ds(start, 16)]

    def ring_peer(step):
        return yh * (RING * CORES) + lax.rem(z + step + RING, RING) * CORES + c

    side = yh * (RING * CORES) + z * CORES + 1 - c

    def section_peer(step):
        return lax.rem(s + step + SECTION, SECTION)

    def cols_of(q, step, d):
        start = q * 512 + (section_peer(step) * NARROW + lax.rem(n - d + NARROW, NARROW)) * 32
        return cols_ref.at[pl.ds(start, 32)]

    ways = ((0, 1), (1, -1))

    def to_section(q, d, block):
        for i, step in ways:
            send(block, block, send_col, recv_x.at[q, d, i], section=section_peer(step))
        if q == 2:
            send(block, block, send_col, recv_xx.at[q, d], section=section_peer(2))

    def begin(q):
        mine = cols_of(q, 0, 0)
        arrived(cols_ref.at[pl.ds(q * 512, 31)], recv_col1.at[q])
        for d in range(1, NARROW):
            send(mine, mine, send_col, recv_y.at[q, d - 1], narrow=lax.rem(n + d, NARROW))
        to_section(q, 0, mine)
        for h in range(2):
            arrived(rows_ref.at[pl.ds(q * 512, 15 + h)], recv_row1.at[q, h])
            block = sub(q, z, c, h)
            for i, step in ways:
                for k in ((1,), (2, 1), (4, 3, 2, 1))[q]:
                    if k < 4 or h == i:
                        send(block, block, send_row, recv_ring.at[q, i, k - 1, h], wide=ring_peer(step * k))
            send(block, block, send_side, recv_side.at[q, 0, 0, h], wide=side)

    def ring_step(q, k):
        for h in range(2):
            for i, step in ways:
                if k == 4 and h != i:
                    continue
                got = sub(q, lax.rem(z - step * k + RING, RING), c, h)
                arrived(got, recv_ring.at[q, i, k - 1, h])
                if q == 0 and (k < 3 or (k == 3 and h == i)):
                    send(got, got, send_row, recv_ring.at[q, i, k, h], wide=ring_peer(step))
                if q == 1 and k == 2:
                    if h == i:
                        send(got, got, send_row, recv_ring.at[q, i, 3, h], wide=ring_peer(2 * step))
                    send(got, got, send_row, recv_ring.at[q, i, 2, h], wide=ring_peer(step))
                send(got, got, send_side, recv_side.at[q, i, k, h], wide=side)

    def from_narrow(q, d):
        got = cols_of(q, 0, d)
        arrived(got, recv_y.at[q, d - 1])
        to_section(q, d, got)

    def along_section(q, d):
        i, step = ways[d % 2]
        got = cols_of(q, -step, d)
        arrived(got, recv_x.at[q, d, i])
        send(got, got, send_col, recv_xx.at[q, d], section=section_peer(step))

    def step(q, k):
        if k == 1:
            from_narrow(q, 1)
        elif k == 2:
            from_narrow(q, 3)
            from_narrow(q, 2)
            along_section(q, 0)
        elif k == 3:
            along_section(q, 1)
        ring_step(q, k)
        if k == 3:
            along_section(q, 3)
            along_section(q, 2)

    def finish(q):
        for d in range(NARROW):
            for i, way in ways:
                if q == 2 or i != d % 2:
                    arrived(cols_of(q, -way, d), recv_x.at[q, d, i])
            arrived(cols_of(q, 2, d), recv_xx.at[q, d])
        for h in range(2):
            arrived(sub(q, z, 1 - c, h), recv_side.at[q, 0, 0, h])
            for k in range(1, 5):
                for i, way in ways:
                    if k == 4 and h != i:
                        continue
                    arrived(sub(q, lax.rem(z - way * k + RING, RING), 1 - c, h), recv_side.at[q, i, k, h])
        lines = rows_ref.reshape(3072, 128)
        for half in range(2):
            left = lines[pl.ds(q * 1024 + half, 512, stride=2), :]
            lh, ll = hi_lo(left.T)
            here = slice(q * 256 + half * 128, q * 256 + half * 128 + 128)
            at_ref[here, 0:512] = lh
            at_ref[here, 512:1024] = lh
            at_ref[here, 1024:1536] = ll
        lines = cols_ref.reshape(1536, 128)
        right = jnp.concatenate(
            [lines[pl.ds(q * 512 + place, 16, stride=32), :] for place in range(32)], axis=0
        )
        rh, rl = hi_lo(right)
        here = slice(q * 128, q * 128 + 128)
        bb_ref[0:512, here] = rh
        bb_ref[512:1024, here] = rl
        bb_ref[1024:1536, here] = rh

    def multiply(q0, q1, c0, c1):
        part = dot(at_ref[q0 * 256 : q1 * 256, :], bb_ref[:, c0 * 128 : c1 * 128])
        for q in range(q0, q1):
            for half in range(2):
                first = (q - q0) * 256 + half * 128
                out_ref[half * 384 + q * 128 : half * 384 + q * 128 + 128, c0 * 128 : c1 * 128] = part[
                    first : first + 128
                ]

    begin(0)
    step(0, 1)
    begin(1)
    step(0, 2)
    step(1, 1)
    begin(2)
    step(0, 3)
    step(1, 2)
    for d in (1, 3, 2):
        from_narrow(2, d)
    step(0, 4)
    step(1, 3)
    finish(0)
    step(1, 4)
    for k in range(1, 5):
        ring_step(2, k)
    finish(1)
    multiply(0, 2, 0, 2)
    finish(2)
    multiply(0, 2, 2, 3)
    multiply(2, 3, 0, 3)
    for copy in sends:
        copy.wait_send()
    for q in range(3):
        arrived(rows_ref.at[pl.ds(q * 512, 31)], send_small)
        arrived(cols_ref.at[pl.ds(q * 512, 31)], send_small)


def polarize(bands, ve, ce, freq, lines, gvec, cy3):
    smem, vmem = pl.BlockSpec(memory_space=pltpu.SMEM), pl.BlockSpec(memory_space=pltpu.VMEM)
    dma = pltpu.SemaphoreType.DMA
    return pl.pallas_call(
        polarize_body,
        out_shape=jax.ShapeDtypeStruct((ROWS, COLS), F32),
        in_specs=[smem] * 4 + [vmem] * 3,
        out_specs=vmem,
        scratch_shapes=[
            pltpu.VMEM((96, 128), jnp.int32),
            pltpu.VMEM((96, 128), jnp.int32),
            pltpu.VMEM((864, 128), F32),
            pltpu.VMEM((256, 896), BF16),
            pltpu.VMEM((48, 2, 128), F32),
            pltpu.VMEM((96, 1, 128), F32),
            pltpu.VMEM((1536, 2, 128), F32),
            pltpu.VMEM((1536, 1, 128), F32),
            pltpu.VMEM((ROWS, 1536), BF16),
            pltpu.VMEM((1536, COLS), BF16),
            dma, dma, dma, dma,
            dma((3, 2)), dma((3,)), dma((3, 2, 4, 2)), dma((3, 2, 5, 2)), dma((3, 3)), dma((3, 4, 2)), dma((3, 4)),
        ],
        compiler_params=pltpu.CompilerParams(
            collective_id=1, has_side_effects=True, vmem_limit_bytes=40 * 1024 * 1024
        ),
        name="polarize",
    )(bands, ve, ce, freq, lines, gvec, cy3)


def on_device(ve_orb, ce_orb, ve, ce, freq, bands, gvec):
    tiles = AREA // 128
    valence = ve_orb.reshape(8, PLANES, tiles, 128).transpose(1, 2, 0, 3).reshape(-1, 128)
    conduction = ce_orb.reshape(PLANES * tiles, 128)
    cx3, bh, bl, cy3 = (jnp.asarray(t) for t in tables())
    lines = exchange(bands.T, valence, conduction, cx3, bh, bl)
    return polarize(bands.T, ve, ce, freq, lines, gvec.reshape(96, 128), cy3)


def solution(mesh):
    in_specs = (
        P(None, "narrow", None),
        P(("section", "wide"), "narrow", None),
        P(),
        P(),
        P(),
        P(("section", "wide"), None),
        P(),
    )
    return jax.shard_map(
        on_device,
        mesh=mesh,
        in_specs=in_specs,
        out_specs=P(("section", "narrow"), "wide"),
        check_vma=False,
    )
```
